32 devices in a mesh: groups: 2 (over x), box: 16 (over z, y, core).
Axes of the slice: x: 2, y: 2, z: 4, core: 2. Of those that a mesh axis runs over, the one named last changes fastest.
Arguments:
- right_sides: float32 [128, 256, 384], P(('groups', 'box')), parts along dimension 0, may hold values from -6 to 6
- blocks: bfloat16 [128, 4, 4, 256, 256], P(('groups', 'box')), parts along dimension 0, may hold values from -0.1875 to 0.1875
- contrast: float32 [8192], P(('groups', 'box')), parts along dimension 0, may hold values from 0.3 to 3
- sample_index: int32 [64, 256], P('box'), may hold values from 0 to 4095
- owners: int32 [64, 4, 4], P('box'), may hold values from 0 to 3, each once within a row
Outputs:
- scattered: float32 [128, 256, 384], P(('groups', 'box')), parts along dimension 0
The draws below stay inside these ranges and needn't reach their ends.
There are 2 independent parts, one for each index of `groups`. The reference program is written for one: setup_inputs(seed, part) draws one part's arguments, and reference() takes and returns one part's arrays. A program takes and returns all parts, laid end to end along the dimension named above; an argument that names none is the same for every part. Nothing has to cross between parts.
Inputs may be any that keep to these rules, and one draw needn't show every extreme that they name: Each row owners[b, m, :] holds every value 0 to 3 once.
All inputs are finite; a program needn't handle non-finite values.
Results may differ from the reference program's by a relative error of at most 0.0093.
Values may be sent and summed in bfloat16 or wider, within the bound.
No kernel may reach another device: no remote copies, remote signals or barrier semaphores. Data moves between devices by JAX's collectives and lax.ppermute only.
A program may use at most 128 MiB of HBM per device.

```python
import math
import jax
import jax.numpy as jnp
import numpy as np
from jax import lax

RADIX = 4
R = 256
LEVELS = 4
COLS = 384
BOXES = 64
CON = 4096
N_BOX = 16


def with_ends(drawn, own_key, low, top_value):
    index_at = [jax.random.randint(jax.random.fold_in(own_key, axis), (), 0, length) for axis, length in enumerate(drawn.shape)]
    main_axis = drawn.shape.index(max(drawn.shape))
    neighbour = index_at[:main_axis] + [(index_at[main_axis] + 1) % drawn.shape[main_axis]] + index_at[main_axis + 1:]
    return drawn.at[tuple(index_at)].set(low).at[tuple(neighbour)].set(top_value)


def level_of(key, extent, shards, smallest, top_value):
    loudness, own = 1.0, jax.random.fold_in(key, 6)
    for position, blocks in shards:
        heights = jnp.exp(jax.random.uniform(jax.random.fold_in(own, position), (blocks,), jnp.float32, smallest / len(shards), top_value / len(shards)))
        loudness = loudness * jnp.repeat(heights, extent[position] // blocks).reshape([-1 if axis == position else 1 for axis in range(len(extent))])
    return loudness


def noise(key, shape, scale, limit, cuts=(), kind=jnp.bfloat16):
    array = jax.random.normal(key, shape, jnp.float32) * scale
    if len(cuts) > 0:
        array = level_of(key, shape, cuts, -0.22, 0.18) * array
    return jnp.clip(array, min=-limit, max=limit).astype(kind)


def setup_inputs(seed: int = 0, part: int = 0) -> dict:
    keys = jax.random.split(jax.random.key(seed), 6)
    part_splits = jax.random.split(jax.random.fold_in(keys[5], part), 6)
    return {
        "right_sides": noise(part_splits[0], (BOXES, R, COLS), 1.0, 6.0, ((0, 16),), jnp.float32),
        "blocks": noise(part_splits[1], (BOXES, LEVELS, RADIX, R, R), (RADIX * R) ** -0.5, 0.1875, ((0, 16),)),
        "contrast": jnp.clip(jnp.exp(math.log(3.0) - 2.3025851 * jax.random.uniform(part_splits[2], (CON,), jnp.float32) ** level_of(part_splits[2], (CON,), ((0, 16),), -0.2, 0.2)), 0.3, 3.0),
        "sample_index": with_ends(jax.random.randint(keys[3], (BOXES, R), 0, CON), jax.random.fold_in(keys[3], 1), 0, CON - 1).astype(jnp.int32),
        "owners": jax.vmap(lambda own: jax.random.permutation(own, RADIX))(jax.random.split(keys[4], BOXES * LEVELS)).reshape((BOXES, LEVELS, RADIX)).astype(jnp.int32),
    }


def box_stride(layer_index, digit_count):
    if layer_index == 0:
        return 1
    return 4 * 4 ** ((layer_index - 1) % digit_count)


def exchange_peer(layer_index, member, digit_count):
    box_ids = np.arange(RADIX * N_BOX)
    spacing = box_stride(layer_index, digit_count)
    digit_now = (box_ids // spacing) % 4
    return (box_ids + (member - digit_now) * spacing).astype(np.int32)


def reference(right_sides, blocks, contrast, sample_index, owners):
    digit_count = 0
    while 4 ** digit_count < N_BOX:
        digit_count += 1
    slots = jnp.arange(RADIX, dtype=jnp.int32)
    current = right_sides
    for layer_index in range(LEVELS):
        rounded = current.astype(jnp.bfloat16).astype(jnp.float32)
        gathered_groups = jnp.stack([rounded[exchange_peer(layer_index, member, digit_count)] for member in range(RADIX)], axis=1)
        indicator_matrix = (owners[:, layer_index, :][:, :, None] == slots[None, None, :]).astype(jnp.float32)
        selected_rows = jnp.einsum("ojg,ojxi->ogxi", indicator_matrix, gathered_groups, precision=lax.Precision.HIGHEST)
        weights = blocks[:, layer_index].astype(jnp.float32)
        current = jnp.einsum("bkrs,bksc->brc", weights, selected_rows, precision=lax.Precision.HIGHEST)
    current = current * contrast[sample_index][:, :, None]
    for layer_index in reversed(range(LEVELS)):
        rounded = current.astype(jnp.bfloat16).astype(jnp.float32)
        weights = blocks[:, layer_index].astype(jnp.float32)
        summand_terms = jnp.einsum("bkrs,brc->bksc", weights, rounded, precision=lax.Precision.HIGHEST)
        indicator_matrix = (owners[:, layer_index, :][:, :, None] == slots[None, None, :]).astype(jnp.float32)
        positioned_rows = jnp.einsum("juo,joym->juym", indicator_matrix, summand_terms, precision=lax.Precision.HIGHEST)
        result = jnp.zeros_like(current)
        for member in range(RADIX):
            result = result.at[exchange_peer(layer_index, member, digit_count)].add(positioned_rows[:, member])
        current = result
    return current
```

```python
import functools

import jax
import jax.numpy as jnp
from jax import lax
from jax.experimental import pallas as pl
from jax.experimental.pallas import tpu as pltpu
from jax.sharding import PartitionSpec as P

CHUNKS = 4


def send(x, step):
    pairs = [(i, step(i)) for i in range(lax.axis_size("box"))]
    return lax.ppermute(x, "box", [(i, j) for i, j in pairs if j is not None])


class Section:
    def __init__(self, low):
        self.low, self.high = low, low + 1
        self.square = low == 0

    def digit(self, i):
        return i >> self.low & 3

    def at(self, i, digit):
        return i & ~(3 << self.low) | digit << self.low

    def flip(self, bits):
        return lambda i: i ^ bits << self.low

    def middle(self, i):
        d = self.digit(i)
        return self.at(i, 3 - d) if d in (1, 2) else None

    def outward(self, i):
        d = self.digit(i)
        return self.at(i, {1: 0, 2: 3}[d]) if d in (1, 2) else None

    def inward(self, i):
        d = self.digit(i)
        return self.at(i, {0: 1, 3: 2}[d]) if d in (0, 3) else None

    def order(self, position):
        d = self.digit(position)
        if self.square:
            return [d, d ^ 1, d ^ 2, d ^ 3]
        left = d < 2
        return [d, d ^ 1, jnp.where(left, 2, 1), jnp.where(left, 3, 0)]

    def gather(self, x):
        if self.square:
            across = send(x, self.flip(2))
            beside = send(x, self.flip(1))
            return [[x], [beside], [across], [send(across, self.flip(1))]]
        near = send(x, self.flip(1))
        b = send(x, self.middle)
        c = send(near, self.middle)
        d = send(b, self.outward)
        e = send(c, self.outward)
        return [[x], [near], [b, d], [c, e]]

    def spread(self, own, outs):
        if self.square:
            pair, across = outs
            got = send(pair, self.flip(1))
            return [own, (got, 0), send(add(across, got[1]), self.flip(2))]
        near, second, third = outs
        e = send(third, self.inward)
        d = send(second, self.inward)
        c = send(add(third, e), self.middle)
        b = send(add(second, d), self.middle)
        return [own, send(add(near, c), self.flip(1)), b]


def add(a, b):
    return (a.astype(jnp.float32) + b.astype(jnp.float32)).astype(jnp.bfloat16)


def dot(a, b):
    return jnp.dot(a, b, preferred_element_type=jnp.float32)


def dot_t(a, b):
    return lax.dot_general(a, b, (((0,), (0,)), ((), ())), preferred_element_type=jnp.float32)


def total(refs):
    acc = refs[0][...].astype(jnp.float32)
    for r in refs[1:]:
        acc = acc + r[...].astype(jnp.float32)
    return acc


def grouped(refs, sizes):
    out, k = [], 0
    for s in sizes:
        out.append(refs[k : k + s])
        k += s
    return out


def one(refs):
    x = refs[0][...]
    for r in refs[1:]:
        x = x + r[...]
    return x.astype(jnp.bfloat16)


def forward_kernel(first, level, sizes, scaled, paired, idx, w, *refs):
    j = first + pl.program_id(0)
    n = sum(sizes)
    groups = grouped(refs[:n], sizes)
    rest = refs[n:]
    acc = None
    for place, group in enumerate(groups):
        term = dot(w[idx[j, level, place]], one(group))
        acc = term if acc is None else acc + term
    if not scaled:
        (out,) = rest
        out[...] = acc.astype(out.dtype)
        return
    scale, *outs = rest
    x = (acc * scale[...]).astype(jnp.bfloat16)
    store_terms(idx, j, level, w, x, outs, paired)


def store_terms(idx, j, level, w, x, outs, paired):
    targets = [outs[0], outs[1].at[0], outs[2], outs[1].at[1]] if paired else outs
    for place in range(4):
        term = dot_t(w[idx[j, level, place]], x)
        targets[place][...] = term.astype(targets[place].dtype)


def adjoint_kernel(first, level, n, paired, idx, w, *refs):
    j = first + pl.program_id(0)
    x = total(refs[:n]).astype(jnp.bfloat16)
    store_terms(idx, j, level, w, x, refs[n:], paired)


def last_kernel(counts, idx, w, *refs):
    out = refs[-1]
    j = 0
    k = 0
    xs = []
    for rows, n in counts:
        for r in range(rows):
            x = None
            for ref in refs[k : k + n]:
                piece = (ref[0, r] if len(ref.shape) == 4 else ref[r]).astype(jnp.float32)
                x = piece if x is None else x + piece
            xs.append(x.astype(jnp.bfloat16))
        k += n
    for place in range(len(xs)):
        acc = None
        for j, x in enumerate(xs):
            term = dot_t(w[j, idx[j, 0, place]], x)
            acc = term if acc is None else acc + term
        out[place] = acc


PARAMS = dict(vmem_limit_bytes=20 * 1024 * 1024)


def per_device(right_sides, blocks, contrast, sample_index, owners):
    n = lax.axis_size("box")
    position = lax.axis_index("box")
    digit_count = (n.bit_length() - 1) // 2
    boxes, rank, cols = right_sides.shape
    levels = blocks.shape[1]
    sections = [None] + [Section(2 * ((m - 1) % digit_count)) for m in range(1, levels)]
    q = jnp.stack(
        [jnp.arange(4, dtype=jnp.int32)]
        + [jnp.stack([jnp.asarray(v, jnp.int32) for v in s.order(position)]) for s in sections[1:]]
    )
    hit = q[None, :, :, None] == jnp.arange(4, dtype=jnp.int32)
    idx = jnp.sum(jnp.where(hit, owners[:, :, None, :], 0), axis=-1)

    table = jnp.where(jnp.arange(n)[:, None] == position, contrast[None, :], 0.0)
    bit = 1
    while bit < n:
        table = table + send(table, lambda i, bit=bit: i ^ bit)
        bit *= 2
    scale = jnp.take(table.reshape(-1), sample_index, axis=0)[:, :, None]

    per = boxes // CHUNKS
    box = pl.BlockSpec((None, rank, cols), lambda j, *_: (j, 0, 0))
    f32 = jax.ShapeDtypeStruct((per, rank, cols), jnp.float32)
    b16 = jax.ShapeDtypeStruct((per, rank, cols), jnp.bfloat16)
    two = jax.ShapeDtypeStruct((2, per, rank, cols), jnp.bfloat16)
    two_spec = pl.BlockSpec((2, None, rank, cols), lambda j, *_: (0, j, 0, 0))

    def w_spec(first, level):
        return pl.BlockSpec(
            (None, None, 4, rank, rank), lambda j, *_: (first + j, level, 0, 0, 0)
        )

    def cost(dots):
        return pl.CostEstimate(
            flops=per * dots * 2 * rank * rank * cols,
            bytes_accessed=per * 4 * rank * (rank + 2 * cols) * 2,
            transcendentals=0,
        )

    def call(kernel, dots, first, level, in_specs, out_specs, out_shape, *args):
        return pl.pallas_call(
            kernel,
            grid_spec=pltpu.PrefetchScalarGridSpec(
                num_scalar_prefetch=1,
                grid=(per,),
                in_specs=[w_spec(first, level)] + in_specs,
                out_specs=out_specs,
            ),
            out_shape=out_shape,
            compiler_params=pltpu.CompilerParams(**PARAMS),
            cost_estimate=cost(dots),
        )(idx, blocks, *args)

    def terms(section):
        if section.square:
            return [box, two_spec, box], [f32, two, b16]
        return [box] * 4, [f32, b16, b16, b16]

    def element(entry):
        if isinstance(entry, tuple):
            array, k = entry
            return array, pl.BlockSpec((None, None, rank, cols), lambda j, *_: (k, j, 0, 0))
        return entry, box

    finals = []
    for c in range(CHUNKS):
        first = c * per
        whole = [
            pl.BlockSpec((None, rank, cols), lambda j, *_, k=k: (k, 0, 0)) for k in range(boxes)
        ]
        x = call(
            functools.partial(forward_kernel, first, 0, [1] * 4, False, False),
            4, first, 0, whole, box, b16, *[right_sides] * boxes,
        )
        for m in range(1, levels):
            section = sections[m]
            groups = section.gather(x)
            sizes = [len(g) for g in groups]
            flat = [a for g in groups for a in g]
            last = m == levels - 1
            kernel = functools.partial(forward_kernel, first, m, sizes, last, section.square)
            specs = [box] * len(flat)
            if not last:
                x = call(kernel, 4, first, m, specs, box, b16, *flat)
                continue
            scale_spec = pl.BlockSpec((None, rank, 1), lambda j, *_: (first + j, 0, 0))
            out_specs, out_shape = terms(section)
            outs = call(kernel, 8, first, m, specs + [scale_spec], out_specs, out_shape, *flat, scale)
        for m in reversed(range(1, levels)):
            section = sections[m]
            parts = section.spread(outs[0], outs[1:])
            if m == 1:
                break
            arrays, specs = zip(*[element(p) for p in parts])
            out_specs, out_shape = terms(sections[m - 1])
            kernel = functools.partial(
                adjoint_kernel, first, m - 1, len(arrays), sections[m - 1].square
            )
            outs = call(kernel, 4, first, m - 1, list(specs), out_specs, out_shape, *arrays)
        finals.append(parts)

    arrays, specs, counts = [], [], []
    for parts in finals:
        for p in parts:
            a, k = p if isinstance(p, tuple) else (p, None)
            arrays.append(a)
            if k is None:
                specs.append(pl.BlockSpec((per, rank, cols), lambda *_: (0, 0, 0)))
            else:
                specs.append(
                    pl.BlockSpec((1, per, rank, cols), lambda *_, k=k: (k, 0, 0, 0))
                )
        counts.append((per, len(parts)))
    return pl.pallas_call(
        functools.partial(last_kernel, counts),
        grid_spec=pltpu.PrefetchScalarGridSpec(
            num_scalar_prefetch=1,
            grid=(1,),
            in_specs=[
                pl.BlockSpec((boxes, None, 4, rank, rank), lambda *_: (0, 0, 0, 0, 0))
            ]
            + specs,
            out_specs=pl.BlockSpec((boxes, rank, cols), lambda *_: (0, 0, 0)),
        ),
        out_shape=jax.ShapeDtypeStruct((boxes, rank, cols), jnp.float32),
        compiler_params=pltpu.CompilerParams(**PARAMS),
        cost_estimate=pl.CostEstimate(
            flops=16 * 2 * rank * rank * cols,
            bytes_accessed=boxes * rank * (4 * rank * 2 + cols * 12),
            transcendentals=0,
        ),
    )(idx, blocks, *arrays)


def solution(mesh):
    return jax.shard_map(
        per_device,
        mesh=mesh,
        in_specs=(
            P(("groups", "box"), None, None),
            P(("groups", "box"), None, None, None, None),
            P(("groups", "box")),
            P("box", None),
            P("box", None, None),
        ),
        out_specs=P(("groups", "box"), None, None),
        check_vma=False,
    )
```

```python
import functools

import jax
import jax.numpy as jnp
from jax import lax
from jax.experimental import pallas as pl
from jax.experimental.pallas import tpu as pltpu
from jax.sharding import PartitionSpec as P


CHUNKS = 4
LEAVE = (0, 1, 2, 3)


def send(x, bits):
    return lax.ppermute(x, "box", [(i, i ^ bits) for i in range(lax.axis_size("box"))])


class Section:
    def __init__(self, low):
        self.low = low
        self.paired = low == 0

    def block(self, owners, j, level, place):
        digit = lax.axis_index("box") >> self.low & 3
        return owners[j, level, digit ^ place]

    def gather(self, x):
        across = send(x, 2 << self.low)
        beside = send(x, 1 << self.low)
        return [x, beside, across, send(across, 1 << self.low)]

    def spread(self, own, outs):
        if self.paired:
            pair, across = outs
            got = send(pair, 1 << self.low)
            total = add(across, got[1])
            return [own, (got, 0), send(total, 2 << self.low)]
        beside, across, corner = outs
        got = send(corner, 1 << self.low)
        far = send(add(across, got), 2 << self.low)
        return [own, send(beside, 1 << self.low), far]


def add(a, b):
    return (a.astype(jnp.float32) + b.astype(jnp.float32)).astype(jnp.bfloat16)


def dot(a, b):
    return jnp.dot(a, b, preferred_element_type=jnp.float32)


def dot_t(a, b):
    return lax.dot_general(a, b, (((0,), (0,)), ((), ())), preferred_element_type=jnp.float32)


def total(refs):
    acc = refs[0][...].astype(jnp.float32)
    for r in refs[1:]:
        acc = acc + r[...].astype(jnp.float32)
    return acc


def entry_kernel(owners, field, blocks, *refs):
    boxes = field.shape[0]
    outs, (x, w, x_sem, w_sem) = refs[:boxes], refs[boxes:]
    x_copy = pltpu.make_async_copy(field, x, x_sem)
    x_copy.start()
    copies = [
        pltpu.make_async_copy(blocks.at[j, 0], w.at[j], w_sem.at[j]) for j in range(boxes)
    ]
    for copy in copies:
        copy.start()
    x_copy.wait()
    rounded = [x[k].astype(jnp.bfloat16) for k in range(boxes)]
    for j in range(boxes):
        copies[j].wait()
        acc = None
        for k in range(boxes):
            term = dot(w[j, owners[j, 0, k]], rounded[k])
            acc = term if acc is None else acc + term
        outs[j][0] = acc.astype(jnp.bfloat16)


def scale_kernel(table, index, out):
    rows, lanes = table.shape
    boxes, rank = index.shape
    high = lax.Precision.HIGHEST
    shift = lanes.bit_length() - 1
    eye = (
        lax.broadcasted_iota(jnp.int32, (rows, rows), 0)
        == lax.broadcasted_iota(jnp.int32, (rows, rows), 1)
    ).astype(jnp.float32)
    for b in range(boxes):
        at = index[b : b + 1, :]
        lane_hit = lax.broadcasted_iota(jnp.int32, (lanes, rank), 0) == (at & (lanes - 1))
        row_hit = lax.broadcasted_iota(jnp.int32, (rows, rank), 0) == (at >> shift)
        picked = lax.dot_general(
            lane_hit.astype(jnp.float32), table[...], (((0,), (1,)), ((), ())),
            precision=high, preferred_element_type=jnp.float32,
        )
        mask = lax.dot_general(
            row_hit.astype(jnp.float32), eye, (((0,), (0,)), ((), ())),
            precision=high, preferred_element_type=jnp.float32,
        )
        out[b] = jnp.sum(picked * mask, axis=1, keepdims=True)


def forward_kernel(section, first, level, scaled, owners, w, *refs):
    j = first + pl.program_id(0)
    rest = refs[4:]
    acc = None
    for place in range(4):
        term = dot(w[section.block(owners, j, level, place)], refs[place][...])
        acc = term if acc is None else acc + term
    if not scaled:
        (out,) = rest
        out[...] = acc.astype(out.dtype)
        return
    scale, *outs = rest
    x = (acc * scale[...]).astype(jnp.bfloat16)
    store_terms(section, owners, j, level, w, x, outs)


def store_terms(section, owners, j, level, w, x, outs):
    targets = [outs[0], outs[1].at[0], outs[2], outs[1].at[1]] if section.paired else outs
    for place in range(4):
        term = dot_t(w[section.block(owners, j, level, place)], x)
        targets[place][...] = term.astype(targets[place].dtype)


def adjoint_kernel(section, first, level, n, owners, w, *refs):
    j = first + pl.program_id(0)
    x = total(refs[:n]).astype(jnp.bfloat16)
    store_terms(section, owners, j, level, w, x, refs[n:])


def exit_kernel(chunks, per, n, owners, w, *refs):
    out = refs[-1]
    xs = []
    for c in range(len(chunks)):
        for r in range(per):
            x = None
            for ref in refs[c * n : (c + 1) * n]:
                piece = (ref[0, r] if len(ref.shape) == 4 else ref[r]).astype(jnp.float32)
                x = piece if x is None else x + piece
            xs.append((chunks[c] * per + r, x.astype(jnp.bfloat16)))
    before = refs[-2] if len(refs) == n * len(chunks) + 2 else None
    for place in range(out.shape[0]):
        acc = None if before is None else before[place]
        for j, x in xs:
            term = dot_t(w[j, owners[j, 0, place]], x)
            acc = term if acc is None else acc + term
        out[place] = acc


ENTRY_VMEM = 62 * 1024 * 1024
PARAMS = dict(vmem_limit_bytes=20 * 1024 * 1024)


def per_device(right_sides, blocks, contrast, sample_index, owners):
    n = lax.axis_size("box")
    position = lax.axis_index("box")
    digit_count = (n.bit_length() - 1) // 2
    boxes, rank, cols = right_sides.shape
    levels = blocks.shape[1]
    sections = [None] + [Section(2 * ((m - 1) % digit_count)) for m in range(1, levels)]

    per = boxes // CHUNKS
    box = pl.BlockSpec((None, rank, cols), lambda j, *_: (j, 0, 0))
    f32 = jax.ShapeDtypeStruct((per, rank, cols), jnp.float32)
    b16 = jax.ShapeDtypeStruct((per, rank, cols), jnp.bfloat16)
    two = jax.ShapeDtypeStruct((2, per, rank, cols), jnp.bfloat16)
    two_spec = pl.BlockSpec((2, None, rank, cols), lambda j, *_: (0, j, 0, 0))

    def cost(dots):
        return pl.CostEstimate(
            flops=dots * 2 * rank * rank * cols,
            bytes_accessed=dots * rank * (rank + 2 * cols) * 2,
            transcendentals=0,
        )

    def call(kernel, dots, first, level, in_specs, out_specs, out_shape, *args):
        return pl.pallas_call(
            kernel,
            grid_spec=pltpu.PrefetchScalarGridSpec(
                num_scalar_prefetch=1,
                grid=(per,),
                in_specs=[
                    pl.BlockSpec(
                        (None, None, 4, rank, rank), lambda j, *_: (first + j, level, 0, 0, 0)
                    )
                ]
                + in_specs,
                out_specs=out_specs,
            ),
            out_shape=out_shape,
            compiler_params=pltpu.CompilerParams(**PARAMS),
            cost_estimate=cost(per * dots),
        )(owners, blocks, *args)

    def terms(section):
        if section.paired:
            return [box, two_spec, box], [f32, two, b16]
        return [box] * 4, [f32, b16, b16, b16]

    def element(entry):
        if isinstance(entry, tuple):
            array, k = entry
            return array, pl.BlockSpec((None, None, rank, cols), lambda j, *_: (k, j, 0, 0))
        return entry, box

    fields = pl.pallas_call(
        entry_kernel,
        grid_spec=pltpu.PrefetchScalarGridSpec(
            num_scalar_prefetch=1,
            grid=(1,),
            in_specs=[pl.BlockSpec(memory_space=pltpu.HBM)] * 2,
            out_specs=[pl.BlockSpec((1, rank, cols), lambda *_: (0, 0, 0))] * boxes,
            scratch_shapes=[
                pltpu.VMEM((boxes, rank, cols), jnp.float32),
                pltpu.VMEM((boxes, 4, rank, rank), jnp.bfloat16),
                pltpu.SemaphoreType.DMA,
                pltpu.SemaphoreType.DMA((boxes,)),
            ],
        ),
        out_shape=[jax.ShapeDtypeStruct((1, rank, cols), jnp.bfloat16)] * boxes,
        compiler_params=pltpu.CompilerParams(vmem_limit_bytes=ENTRY_VMEM),
        cost_estimate=cost(4 * boxes),
    )(owners, right_sides, blocks)

    table = jnp.where(jnp.arange(n)[:, None] == position, contrast[None, :], 0.0)
    bit = 1
    while bit < n:
        got = send(table, bit)
        table = table + got
        bit *= 2
    scale = pl.pallas_call(
        scale_kernel,
        out_shape=jax.ShapeDtypeStruct((boxes, rank, 1), jnp.float32),
        compiler_params=pltpu.CompilerParams(**PARAMS),
    )(table, sample_index)

    finals = []
    for c in range(CHUNKS):
        first = c * per
        x = fields[first] if per == 1 else jnp.concatenate(fields[first : first + per])
        for m in range(1, levels):
            section = sections[m]
            flat = section.gather(x)
            last = m == levels - 1
            kernel = functools.partial(forward_kernel, section, first, m, last)
            specs = [box] * 4
            if not last:
                x = call(kernel, 4, first, m, specs, box, b16, *flat)
                continue
            scale_spec = pl.BlockSpec((None, rank, 1), lambda j, *_: (first + j, 0, 0))
            out_specs, out_shape = terms(section)
            outs = call(
                kernel, 8, first, m, specs + [scale_spec], out_specs, out_shape,
                *flat, scale,
            )
        for m in reversed(range(1, levels)):
            parts = sections[m].spread(outs[0], outs[1:])
            if m == 1:
                break
            section = sections[m - 1]
            arrays, specs = zip(*[element(p) for p in parts])
            out_specs, out_shape = terms(section)
            kernel = functools.partial(adjoint_kernel, section, first, m - 1, len(arrays))
            outs = call(kernel, 4, first, m - 1, list(specs), out_specs, out_shape, *arrays)
        finals.append(parts)

    def leave(chunks, before):
        arrays, specs = [], []
        for c in chunks:
            for p in finals[c]:
                a, k = p if isinstance(p, tuple) else (p, None)
                arrays.append(a)
                if k is None:
                    specs.append(pl.BlockSpec((per, rank, cols), lambda *_: (0, 0, 0)))
                else:
                    specs.append(
                        pl.BlockSpec((1, per, rank, cols), lambda *_, k=k: (k, 0, 0, 0))
                    )
        whole = pl.BlockSpec((boxes, rank, cols), lambda *_: (0, 0, 0))
        if before is not None:
            arrays.append(before)
            specs.append(whole)
        return pl.pallas_call(
            functools.partial(exit_kernel, chunks, per, len(finals[0])),
            grid_spec=pltpu.PrefetchScalarGridSpec(
                num_scalar_prefetch=1,
                grid=(1,),
                in_specs=[pl.BlockSpec((boxes, None, 4, rank, rank), lambda *_: (0, 0, 0, 0, 0))]
                + specs,
                out_specs=whole,
            ),
            out_shape=jax.ShapeDtypeStruct((boxes, rank, cols), jnp.float32),
            compiler_params=pltpu.CompilerParams(**PARAMS),
            cost_estimate=cost(4 * len(chunks)),
        )(owners, blocks, *arrays)

    sums = leave(LEAVE[:-1], None)
    return leave(LEAVE[-1:], sums)


def solution(mesh):
    return jax.shard_map(
        per_device,
        mesh=mesh,
        in_specs=(
            P(("groups", "box"), None, None),
            P(("groups", "box"), None, None, None, None),
            P(("groups", "box")),
            P("box", None),
            P("box", None, None),
        ),
        out_specs=P(("groups", "box"), None, None),
        check_vma=False,
    )
```
